256 devices in a mesh: seq: 16 (over z_lo, x), tp: 8 (over y, core), grp: 2 (over z_hi).
Axes of the slice: x: 4, y: 4, z: 8 (z_hi: 2, z_lo: 4; z = z_hi * 4 + z_lo), core: 2. Of those that a mesh axis runs over, the one named last changes fastest.
Arguments:
- prefill_query: bfloat16 [2, 6144, 8192], P('grp', 'seq', 'tp'), may hold values from -6 to 6
- prefill_keys: bfloat16 [2, 6144, 1024], P('grp', 'seq', 'tp'), may hold values from -6 to 6
- prefill_values: bfloat16 [2, 6144, 1024], P('grp', 'seq', 'tp'), may hold values from -6 to 6
- decode_query: bfloat16 [2, 128, 4, 8192], P('grp', 'seq', None, 'tp'), may hold values from -6 to 6
- decode_keys: bfloat16 [2, 128, 4, 1024], P('grp', 'seq', None, 'tp'), may hold values from -6 to 6
- decode_values: bfloat16 [2, 128, 4, 1024], P('grp', 'seq', None, 'tp'), may hold values from -6 to 6
- page_table: int32 [2, 128, 16], P('grp', 'seq'), may hold values from 0 to 47
- context_lengths: int32 [2, 128], P('grp', 'seq'), may hold values from 1 to 2048
- check_rows: bfloat16 [8, 128], replicated, may hold values from -0.125 to 0.125
Outputs:
- prefill_out: bfloat16 [2, 6144, 8192], P('grp', 'seq', 'tp')
- decode_out: bfloat16 [2, 128, 4, 8192], P('grp', 'seq', None, 'tp')
- page_digest: float32 [2, 128, 8, 2048], P('grp', 'seq', None, 'tp')
The draws below stay inside these ranges and needn't reach their ends.
Inputs may be any that keep to these rules, and one draw needn't show every extreme that they name: page_table[g, r, j] names the page of 128 tokens of prompt 1 - g that holds context tokens j * 128 to j * 128 + 127 of request r; pages may repeat. Request r reads its first context_lengths[g, r] context tokens.
All inputs are finite; a program needn't handle non-finite values.
Results may differ from the reference program's by a relative error of at most 0.014.
Values may be sent and summed in bfloat16 or wider, within the bound.
No kernel may reach another device: no remote copies, remote signals or barrier semaphores. Data moves between devices by JAX's collectives and lax.ppermute only.
A program may use at most 64 MiB of HBM per device.

```python
import math
import jax
import jax.numpy as jnp
from jax import lax

HQ = 64
KVH = 8
HD = 128
PAGE = 128
MAXPAGES = 16
STEPS = 4
CSW = 8
PROMPT = 6144
NPAGES = 48
MAXCTX = 2048
REQS = 128


def drawn_normal(key, shape):
    return jax.random.truncated_normal(key, -6.0, 6.0, shape, jnp.float32)


def draw_prefill_query(key, part):
    values = drawn_normal(jax.random.fold_in(key, 11), (2, PROMPT, HQ * HD))
    return values.astype(jnp.bfloat16)


def draw_prefill_keys(key, part):
    values = drawn_normal(jax.random.fold_in(key, 12), (2, PROMPT, KVH * HD))
    return values.astype(jnp.bfloat16)


def draw_decode_query(key, part):
    values = drawn_normal(jax.random.fold_in(key, 13), (2, REQS, STEPS, HQ * HD))
    return values.astype(jnp.bfloat16)


def draw_decode_keys(key, part):
    values = drawn_normal(jax.random.fold_in(key, 14), (2, REQS, STEPS, KVH * HD))
    return values.astype(jnp.bfloat16)


def touch_ends(result, stream_key, low, high):
    shape = result.shape
    index_at = [jax.random.randint(jax.random.fold_in(stream_key, axis), (), 0, shape[axis]) for axis in range(len(shape))]
    result = result.at[tuple(index_at)].set(low)
    longest = shape.index(max(shape))
    index_at[longest] = (index_at[longest] + 1) % shape[longest]
    return result.at[tuple(index_at)].set(high)


def steps_of(own_key, dims, split, least, high):
    def one(position, shards_of):
        heights = jax.random.uniform(jax.random.fold_in(jax.random.fold_in(own_key, 6), position), (shards_of,), jnp.float32, least / len(split), high / len(split))
        return jnp.repeat(jnp.exp(heights), dims[position] // shards_of).reshape((-1,) + (1,) * (len(dims) - position - 1))

    factor_of = one(*split[0])
    for cut in split[1:]:
        factor_of = factor_of * one(*cut)
    return factor_of


def bell_draw(stream_key, extent, deviation, reach, split=(), kind=jnp.bfloat16):
    level = steps_of(stream_key, extent, split, -0.22, 0.18) if split else 1.0
    values = jax.random.normal(stream_key, extent, jnp.float32) * deviation * level
    return jnp.minimum(jnp.maximum(values, -reach), reach).astype(kind)


def setup_inputs(seed: int = 0) -> dict:
    streams_of = jax.random.split(jax.random.key(seed), 10)
    return {
        "prefill_query": draw_prefill_query(jax.random.fold_in(streams_of[9], 71), 0),
        "prefill_keys": draw_prefill_keys(jax.random.fold_in(streams_of[9], 71), 0),
        "prefill_values": bell_draw(streams_of[2], (2, PROMPT, KVH * HD), 1.0, 6.0, ((0, 2), (1, 16), (2, 8))),
        "decode_query": draw_decode_query(jax.random.fold_in(streams_of[9], 71), 0),
        "decode_keys": draw_decode_keys(jax.random.fold_in(streams_of[9], 71), 0),
        "decode_values": bell_draw(streams_of[5], (2, REQS, STEPS, KVH * HD), 1.0, 6.0, ((0, 2), (1, 16), (3, 8))),
        "page_table": touch_ends(jax.random.randint(streams_of[6], (2, REQS, MAXPAGES), 0, NPAGES), jax.random.fold_in(streams_of[6], 1), 0, NPAGES - 1).astype(jnp.int32),
        "context_lengths": touch_ends(jax.random.randint(streams_of[7], (2, REQS), 1, MAXCTX + 1), jax.random.fold_in(streams_of[7], 1), 1, MAXCTX).astype(jnp.int32),
        "check_rows": bell_draw(streams_of[8], (CSW, PAGE), MAXCTX ** -0.5, 0.125),
    }


def rounded(weights):
    return lax.optimization_barrier(weights.astype(jnp.bfloat16)).astype(jnp.float32)

def prompt_attention(query_rows, key_rows, value_rows):
    groups = HQ // KVH
    block_rows = math.gcd(128, PROMPT)
    score_scale = 1.0 / math.sqrt(HD)
    blocks = query_rows.reshape(PROMPT // block_rows, block_rows, KVH, groups, HD)
    key_heads = key_rows.reshape(PROMPT, KVH, HD).astype(jnp.float32)
    value_heads = value_rows.reshape(PROMPT, KVH, HD).astype(jnp.float32)
    columns = jnp.arange(PROMPT, dtype=jnp.int32)

    def one_block(block_pair):
        query_block, block_index = block_pair
        scores = jnp.einsum('rkgd,ckd->kgrc', query_block.astype(jnp.float32), key_heads) * score_scale
        places = block_index * block_rows + jnp.arange(block_rows, dtype=jnp.int32)
        allowed = columns[None, :] <= places[:, None]
        scores = jnp.where(allowed, scores, -jnp.inf)
        row_max = lax.optimization_barrier(jnp.max(scores, axis=-1, keepdims=True))
        weights = jnp.where(allowed, jnp.exp(scores - row_max), 0.0)
        row_total = lax.optimization_barrier(jnp.sum(weights, axis=-1))
        mixed = jnp.einsum('kgrc,ckd->rkgd', rounded(weights), value_heads)
        mixed = mixed / jnp.transpose(row_total, (2, 0, 1))[..., None]
        return mixed.reshape(block_rows, HQ * HD).astype(jnp.bfloat16)
    outputs = lax.map(one_block, (blocks, jnp.arange(PROMPT // block_rows, dtype=jnp.int32)))
    return outputs.reshape(PROMPT, HQ * HD)

def decode_group(query, new_keys, new_values, own_table, lengths, key_rows, value_rows, check_rows):
    groups = HQ // KVH
    score_scale = 1.0 / math.sqrt(HD)
    offsets = jnp.arange(PAGE, dtype=jnp.int32)
    positions = jnp.arange(MAXCTX, dtype=jnp.int32)
    step_order = jnp.arange(STEPS, dtype=jnp.int32)
    causal = step_order[None, :] <= step_order[:, None]
    check_full = jnp.tile(check_rows.astype(jnp.float32), (1, MAXPAGES))

    def one_request(request_items):
        query_rows, fresh_keys, fresh_values, table_row, length = request_items
        token_index = (table_row[:, None] * PAGE + offsets[None, :]).reshape(MAXCTX).astype(jnp.int32)
        context_keys = key_rows[token_index].reshape(MAXCTX, KVH, HD).astype(jnp.float32)
        context_values = value_rows[token_index].reshape(MAXCTX, KVH, HD).astype(jnp.float32)
        live = positions < length
        query_heads = query_rows.reshape(STEPS, KVH, groups, HD).astype(jnp.float32)
        old_scores = jnp.einsum('skgd,tkd->skgt', query_heads, context_keys) * score_scale
        old_scores = jnp.where(live[None, None, None, :], old_scores, -jnp.inf)
        fresh_heads = fresh_keys.reshape(STEPS, KVH, HD).astype(jnp.float32)
        fresh_scores = jnp.einsum('skgd,jkd->skgj', query_heads, fresh_heads) * score_scale
        fresh_scores = jnp.where(causal[:, None, None, :], fresh_scores, -jnp.inf)
        joint_max = jnp.maximum(lax.optimization_barrier(jnp.max(old_scores, axis=-1)), lax.optimization_barrier(jnp.max(fresh_scores, axis=-1)))[..., None]
        old_weights = jnp.where(live[None, None, None, :], jnp.exp(old_scores - joint_max), 0.0)
        fresh_weights = jnp.where(causal[:, None, None, :], jnp.exp(fresh_scores - joint_max), 0.0)
        totals = lax.optimization_barrier(jnp.sum(old_weights, axis=-1)) + lax.optimization_barrier(jnp.sum(fresh_weights, axis=-1))
        mixed = jnp.einsum('skgt,tkd->skgd', rounded(old_weights), context_values)
        fresh_value_heads = fresh_values.reshape(STEPS, KVH, HD).astype(jnp.float32)
        mixed = mixed + jnp.einsum('skgj,jkd->skgd', rounded(fresh_weights), fresh_value_heads)
        output = (mixed / totals[..., None]).reshape(STEPS, HQ * HD).astype(jnp.bfloat16)
        check_live = check_full * live[None, :].astype(jnp.float32)
        paired = jnp.concatenate([context_keys, context_values], axis=-1)
        digest = jnp.einsum('ct,tke->cke', check_live, paired, precision=lax.Precision.HIGHEST)
        return (output, digest.reshape(CSW, KVH * 2 * HD))
    return lax.map(one_request, (query, new_keys, new_values, own_table, lengths))

def reference(prefill_query, prefill_keys, prefill_values, decode_query, decode_keys, decode_values, page_table, context_lengths, check_rows):
    prefill_out = jnp.stack([prompt_attention(prefill_query[0], prefill_keys[0], prefill_values[0]), prompt_attention(prefill_query[1], prefill_keys[1], prefill_values[1])])
    outputs = []
    digests = []
    for group in range(2):
        output, digest = decode_group(decode_query[group], decode_keys[group], decode_values[group], page_table[group], context_lengths[group], prefill_keys[1 - group], prefill_values[1 - group], check_rows)
        outputs.append(output)
        digests.append(digest)
    return (prefill_out, jnp.stack(outputs), jnp.stack(digests))
```

```python
import math

import jax
import jax.numpy as jnp
from jax import lax
from jax.experimental import pallas as pl
from jax.experimental.pallas import tpu as pltpu
from jax.sharding import Mesh
from jax.sharding import PartitionSpec as P


HD = 128
PAGE = 128
ROWS = 384
HEADS = 8
REQ = 8
STEPS = 4
SLOTS = 16
CSW = 8
QROWS = HEADS * REQ * STEPS
SCALE = math.log2(math.e) / math.sqrt(HD)
LOW = -1e30
LARGE = 2.0**100
SEQ = ("z", "x")
STATE = (HEADS, ROWS, HD)
PAIR = 2

f32 = jnp.float32
bf16 = jnp.bfloat16


def dot_t(a, b):
    return lax.dot_general(a, b, (((1,), (1,)), ((), ())), preferred_element_type=f32)


def dot(a, b):
    return lax.dot_general(a, b, (((1,), (0,)), ((), ())), preferred_element_type=f32)


SMALL = pltpu.CompilerParams(vmem_limit_bytes=8 << 20)


def smem():
    return pl.BlockSpec(memory_space=pltpu.SMEM)


def prepare_body(length, query, table, new_keys, new_values, out, m_out, l_out, a_out, wide):
    for g in range(HEADS):
        out[g * 32 : (g + 1) * 32, :] = query[:, :, g * HD : (g + 1) * HD].astype(f32).reshape(32, HD).astype(bf16)
    wide[...] = jnp.zeros((REQ, HD), jnp.int32)
    wide[:, :SLOTS] = table[...]
    lane = lax.broadcasted_iota(jnp.int32, (REQ, HD), 1)
    line = lax.broadcasted_iota(jnp.int32, (REQ, HD), 0)
    tokens = jnp.zeros((REQ, HD), jnp.int32)
    for r in range(REQ):
        tokens = jnp.where(line == r, length[0, r], tokens)
    limit = jnp.clip(tokens - (lane - SLOTS) * PAGE, 0, PAGE)
    facts = jnp.where(lane < SLOTS, wide[...], jnp.where(lane < 2 * SLOTS, limit, 0))
    facts = jnp.concatenate([facts.astype(f32), jnp.zeros((8, HD), f32)], axis=0)
    out[QROWS:, :] = facts.astype(bf16)
    s = dot_t(out[:QROWS, :], new_keys[...]) * SCALE
    row = lax.broadcasted_iota(jnp.int32, (QROWS, 32), 0) % 32
    col = lax.broadcasted_iota(jnp.int32, (QROWS, 32), 1)
    seen = (row // STEPS == col // STEPS) & (col <= row)
    s = jnp.where(seen, s, LOW)
    top = jnp.max(s, axis=1, keepdims=True)
    w = jnp.exp2(s - top)
    m_out[...] = jnp.broadcast_to(top, (QROWS, HD))
    l_out[...] = jnp.broadcast_to(jnp.sum(w, axis=1, keepdims=True), (QROWS, HD))
    a_out[...] = dot(w.astype(bf16), new_values[...])


def prepare(query, table, length, new_keys, new_values):
    vmem = pl.BlockSpec(memory_space=pltpu.VMEM)
    return pl.pallas_call(
        prepare_body,
        in_specs=[smem()] + [vmem] * 4,
        out_specs=(vmem,) * 4,
        out_shape=(jax.ShapeDtypeStruct((QROWS + 16, HD), bf16),) + (jax.ShapeDtypeStruct((QROWS, HD), f32),) * 3,
        scratch_shapes=[pltpu.VMEM((REQ, HD), jnp.int32)],
        compiler_params=SMALL,
        name="prepare",
    )(length, query, table, new_keys, new_values)


class Block:
    def __init__(self, key_ref, key_col, value_ref, value_col, n=None):
        self.parts = ((key_ref, key_col), (value_ref, value_col))
        self.n = n

    def rows(self, which, start, stop):
        ref, col = self.parts[which]
        if self.n is None:
            return ref[start:stop, col * HD : (col + 1) * HD]
        return ref[self.n, start:stop, col * HD : (col + 1) * HD]

    def key(self):
        return self.rows(0, 0, ROWS)

    def value(self):
        return self.rows(1, 0, ROWS)


def chunks_of(blocks):
    half = [(b, i * HD) for b in blocks for i in range(ROWS // HD)]
    for i in range(0, len(half), 2):
        some = half[i : i + 2]
        yield tuple(
            jnp.concatenate([b.rows(which, r, r + HD) for b, r in some], axis=0) for which in (0, 1)
        )


def fold_fixed(before, after, h, q, blocks):
    level = before[0][h]
    total = before[1][h]
    mixed = before[2][h]
    for k, v in chunks_of(blocks):
        scores = dot_t(q(), k)
        weights = [jnp.exp2(scores[:, i : i + HD] * SCALE - level) for i in range(0, scores.shape[1], HD)]
        for w in weights:
            total = total + w
        mixed = mixed + dot(jnp.concatenate([w.astype(bf16) for w in weights], axis=1), v)
    after[1][h] = total
    after[2][h] = mixed


def fold_moving(before, after, h, q, blocks):
    m_ref, l_ref, a_ref = after

    @pl.loop(0, ROWS // HD)
    def _(i):
        rows = pl.ds(pl.multiple_of(i * HD, HD), HD)
        l_ref[h, rows] = before[1][h, rows]
        a_ref[h, rows] = before[2][h, rows]
        for b in blocks:
            scores = dot_t(q(rows), b.key()) * SCALE
            level = m_ref[h, rows]
            now = jnp.maximum(level, jnp.max(scores, axis=1, keepdims=True))
            fade = jnp.exp2(level - now)
            weights = [jnp.exp2(scores[:, j : j + HD] - now) for j in range(0, ROWS, HD)]
            m_ref[h, rows] = now
            l_ref[h, rows] = l_ref[h, rows] * fade + (weights[0] + weights[1] + weights[2])
            update = dot(jnp.concatenate([w.astype(bf16) for w in weights], axis=1), b.value())
            a_ref[h, rows] = a_ref[h, rows] * fade + update


def too_large(l_ref):
    top = l_ref[0]
    for h in range(1, HEADS):
        top = jnp.maximum(top, l_ref[h])
    return jnp.max(top) > LARGE


def fold_own(state, h, q, own):
    m_ref, l_ref, a_ref = state
    scores = dot_t(q(), own.key()) * SCALE
    row = lax.broadcasted_iota(jnp.int32, (ROWS, ROWS), 0)
    col = lax.broadcasted_iota(jnp.int32, (ROWS, ROWS), 1)
    scores = jnp.where(col <= row, scores, LOW)
    now = jnp.max(scores, axis=1, keepdims=True)
    weights = jnp.exp2(scores - now)
    m_ref[h] = jnp.broadcast_to(now, (ROWS, HD))
    l_ref[h] = weights[:, :HD] + weights[:, HD : 2 * HD] + weights[:, 2 * HD :]
    a_ref[h] = dot(weights.astype(bf16), own.value())


def cost(blocks):
    n = HEADS * ROWS * ROWS * blocks
    return pl.CostEstimate(flops=4 * n * HD, bytes_accessed=1 << 20, transcendentals=n)


def part(groups, place, query, arrays, state=None, last=False, own=None, weight=4):
    count = len(arrays)
    carried = [] if state is None else list(state)

    def body(place_ref, q_ref, *refs):
        blocks = refs[:count]
        before = refs[count : count + len(carried)]
        after = refs[count + len(carried) :]
        out = None
        if last:
            out, after = after[0], (before[0],) + tuple(after[1:])
        cases = groups(blocks)
        z, x = place_ref[0], place_ref[1]

        def query_of(h):
            lanes = pl.ds(pl.multiple_of(h * HD, HD), HD)
            return lambda rows=slice(None): q_ref[rows, lanes]

        def run(folded, slow):
            if own is not None:

                @pl.loop(0, HEADS // PAIR)
                def _(i):
                    for n in range(PAIR):
                        h = i * PAIR + n
                        fold_own(after, h, query_of(h), own(blocks))

            source = after if own is not None else before
            idle = None
            for holds, step, some in cases:
                held = holds(z, x)
                idle = held if idle is None else idle | held
                if slow:
                    step = 1

                @pl.when(held)
                def _(some=some, step=step):
                    @pl.loop(0, HEADS // step)
                    def _(i):
                        for n in range(step):
                            h = i * step + n
                            folded(source, after, h, query_of(h), some)

            if own is None:

                @pl.when(jnp.logical_not(idle))
                def _():
                    @pl.loop(0, HEADS)
                    def _(h):
                        after[1][h] = before[1][h]
                        after[2][h] = before[2][h]

        run(fold_fixed, False)

        @pl.when(too_large(after[1]))
        def _():
            run(fold_moving, True)

        if last:

            @pl.loop(0, HEADS)
            def _(h):
                total = jnp.sum(after[1][h], axis=1, keepdims=True)
                out[:, pl.ds(pl.multiple_of(h * HD, HD), HD)] = (after[2][h] / total).astype(bf16)

    vmem = pl.BlockSpec(memory_space=pltpu.VMEM)
    shape = jax.ShapeDtypeStruct(STATE, f32)
    if last:
        how = dict(
            out_specs=vmem,
            out_shape=jax.ShapeDtypeStruct((ROWS, HEADS * HD), bf16),
            scratch_shapes=[pltpu.VMEM(STATE, f32)] * 2,
        )
    else:
        how = dict(
            out_specs=(vmem,) * 3,
            out_shape=(shape,) * 3,
            input_output_aliases={2 + count: 0} if carried else {},
        )
    return pl.pallas_call(
        body,
        in_specs=[smem()] + [vmem] * (1 + count + len(carried)),
        compiler_params=pltpu.CompilerParams(vmem_limit_bytes=20 << 20),
        cost_estimate=cost(weight),
        **how,
    )(place, query, *arrays, *carried)


def count_body(ask, check, each_out, weighted_out, n_ref):
    facts = ask[QROWS : QROWS + 16, :].astype(f32)[:REQ]
    lane = lax.broadcasted_iota(jnp.int32, (REQ, HD), 1).astype(f32)
    named = [jnp.broadcast_to(facts[:, j : j + 1], (REQ, HD)) for j in range(SLOTS)]
    fits = [jnp.where(lane < facts[:, SLOTS + j : SLOTS + j + 1], 1.0, 0.0) for j in range(SLOTS)]
    checks = check[...].astype(f32)
    upper = lax.broadcasted_iota(jnp.int32, (8, HD), 0) < STEPS

    @pl.loop(0, 16)
    def _(b):
        for i in range(ROWS // PAGE):
            page = (b * (ROWS // PAGE) + i).astype(f32)
            n = jnp.zeros((REQ, HD), f32)
            for j in range(SLOTS):
                n = n + jnp.where(named[j] == page, fits[j], 0.0)
            n_ref[...] = n
            lines = [jnp.broadcast_to(n_ref[r : r + 1, :], (8, HD)) for r in range(REQ)]
            for r in range(0, REQ, 2):
                each_out[b, r * 4 : r * 4 + 8, i * HD : (i + 1) * HD] = jnp.where(upper, lines[r], lines[r + 1])
                both = jnp.concatenate([lines[r] * checks, lines[r + 1] * checks], axis=0)
                weighted_out[b, r * 8 : r * 8 + 16, i * HD : (i + 1) * HD] = both.astype(bf16)


def count_part(ask, check):
    return pl.pallas_call(
        count_body,
        out_shape=(
            jax.ShapeDtypeStruct((16, 32, ROWS), f32),
            jax.ShapeDtypeStruct((16, REQ * CSW, ROWS), bf16),
        ),
        scratch_shapes=[pltpu.VMEM((REQ, HD), f32)],
        compiler_params=SMALL,
        cost_estimate=pl.CostEstimate(flops=1 << 24, bytes_accessed=2 << 20, transcendentals=0),
        name="count",
    )(ask, check)


def context_body(blocks_of, count, place, ask, each_ref, weighted_ref, *refs):
    held = blocks_of(refs[:count])
    out, m_ref, l_ref, a_ref, s_ref = refs[count:]
    z, x = place[0], place[1]
    q = ask[:QROWS, :]

    def index(dz, dx):
        return ((z + 4 - dz) % 4) * 4 + (x + 4 - dx) % 4

    def apply(dz, dx, block):
        b = index(dz, dx)
        scores = dot_t(q, block.key()) * SCALE
        each = jnp.concatenate([each_ref[b]] * HEADS, axis=0)
        return b, scores, each

    level = jnp.max(dot_t(q, held[0][2].key()), axis=1, keepdims=True) * SCALE
    level = jnp.maximum(jnp.full((QROWS, HD), LOW), level)
    total = jnp.zeros((QROWS, HD), f32)
    mixed = jnp.zeros((QROWS + REQ * CSW, HD), f32)
    digest_k = jnp.zeros((REQ * CSW, HD), f32)
    for dz, dx, block in held:
        b, scores, each = apply(dz, dx, block)
        weights = [
            jnp.exp2(scores[:, i : i + HD] - level) * each[:, i : i + HD] for i in range(0, ROWS, HD)
        ]
        total = total + (weights[0] + weights[1] + weights[2])
        weighted = weighted_ref[b]
        left = jnp.concatenate([jnp.concatenate([w.astype(bf16) for w in weights], axis=1), weighted], axis=0)
        mixed = mixed + dot(left, block.value())
        digest_k = digest_k + dot(weighted, block.key())
    m_ref[...] = level
    l_ref[...] = jnp.broadcast_to(jnp.sum(total, axis=1, keepdims=True), (QROWS, HD))
    a_ref[...] = mixed
    spread = l_ref[...]

    @pl.when(jnp.logical_not((jnp.max(spread) < LARGE) & (jnp.min(spread) > 1 / LARGE)))
    def _():
        @pl.loop(0, HEADS)
        def _(g):
            rows = pl.ds(pl.multiple_of(g * 32, 32), 32)
            top = jnp.full((32, HD), LOW)
            for n, (dz, dx, block) in enumerate(held):
                scores = dot_t(ask[rows, :], block.key()) * SCALE
                scores = jnp.where(each_ref[index(dz, dx)] > 0, scores, LOW)
                s_ref[n] = scores
                top = jnp.maximum(top, jnp.max(scores, axis=1, keepdims=True))
            total = jnp.zeros((32, HD), f32)
            mixed = jnp.zeros((32, HD), f32)
            for n, (dz, dx, block) in enumerate(held):
                weights = jnp.exp2(s_ref[n] - top[:, :1]) * each_ref[index(dz, dx)]
                total = total + jnp.sum(weights, axis=1, keepdims=True)
                mixed = mixed + dot(weights.astype(bf16), block.value())
            m_ref[rows, :] = top
            l_ref[rows, :] = total
            a_ref[rows, :] = mixed

    total = l_ref[...]
    out[:QROWS, :] = (a_ref[:QROWS, :] / total).astype(bf16)
    out[QROWS : QROWS + 64, :] = digest_k.astype(bf16)
    out[QROWS + 64 : QROWS + 128, :] = a_ref[QROWS:, :].astype(bf16)
    top = m_ref[...] + jnp.log2(total)
    diagonal = lax.broadcasted_iota(jnp.int32, (HD, HD), 0) == lax.broadcasted_iota(jnp.int32, (HD, HD), 1)
    line = lax.broadcasted_iota(jnp.int32, (16, HD), 0)
    packed = jnp.zeros((16, HD), f32)
    for i in range(2):
        rest = jnp.sum(jnp.where(diagonal, top[i * HD : (i + 1) * HD], 0.0), axis=0, keepdims=True)
        for n in range(3):
            piece = rest.astype(bf16).astype(f32)
            packed = jnp.where(line == 2 * n + i, jnp.broadcast_to(piece, (16, HD)), packed)
            rest = rest - piece
    out[QROWS + 128 :, :] = packed.astype(bf16)


def context_part(place, ask, each, weighted, arrays, blocks_of):
    vmem = pl.BlockSpec(memory_space=pltpu.VMEM)
    return pl.pallas_call(
        lambda *refs: context_body(blocks_of, len(arrays), *refs),
        in_specs=[smem()] + [vmem] * (3 + len(arrays)),
        out_specs=vmem,
        out_shape=jax.ShapeDtypeStruct((QROWS + 144, HD), bf16),
        scratch_shapes=[
            pltpu.VMEM((QROWS, HD), f32),
            pltpu.VMEM((QROWS, HD), f32),
            pltpu.VMEM((QROWS + REQ * CSW, HD), f32),
            pltpu.VMEM((16, 32, ROWS), f32),
        ],
        compiler_params=pltpu.CompilerParams(vmem_limit_bytes=20 << 20),
        cost_estimate=pl.CostEstimate(
            flops=4 * QROWS * 16 * ROWS * HD, bytes_accessed=4 << 20, transcendentals=QROWS * 16 * ROWS
        ),
        name="context",
    )(place, ask, each, weighted, *arrays)


def finish_body(back, m_ref, l_ref, a_ref, out, digest):
    diagonal = lax.broadcasted_iota(jnp.int32, (HD, HD), 0) == lax.broadcasted_iota(jnp.int32, (HD, HD), 1)
    tail = back[QROWS + 128 :, :].astype(f32)
    level = []
    for i in range(2):
        line = tail[i : i + 1] + tail[2 + i : 3 + i] + tail[4 + i : 5 + i]
        spread = jnp.where(diagonal, jnp.broadcast_to(line, (HD, HD)), 0.0)
        level.append(jnp.sum(spread, axis=1, keepdims=True))
    level = jnp.concatenate(level, axis=0)
    new = m_ref[...]
    joint = jnp.maximum(level, new)
    old = jnp.exp2(level - joint)
    new = jnp.exp2(new - joint)
    mixed = back[:QROWS, :].astype(f32) * old + a_ref[...] * new
    mixed = mixed / (old + l_ref[...] * new)
    for g in range(HEADS):
        out[:, :, g * HD : (g + 1) * HD] = mixed[g * 32 : (g + 1) * 32].reshape(REQ, STEPS, HD).astype(bf16)
    digest[:, :HD] = back[QROWS : QROWS + 64, :].astype(f32)
    digest[:, HD:] = back[QROWS + 64 : QROWS + 128, :].astype(f32)


def finish(back, fresh):
    return pl.pallas_call(
        finish_body,
        out_shape=(
            jax.ShapeDtypeStruct((REQ, STEPS, HEADS * HD), bf16),
            jax.ShapeDtypeStruct((REQ * CSW, 2 * HD), f32),
        ),
        compiler_params=SMALL,
        name="finish",
    )(back, *fresh)


def turn(shard, axis, by):
    n = lax.axis_size(axis)
    return lax.ppermute(shard, axis, [(i, (i + by) % n) for i in range(n)])


def swap(shard):
    return lax.ppermute(shard, "grp", [(0, 1), (1, 0)])


def work(
    prefill_query,
    prefill_keys,
    prefill_values,
    decode_query,
    decode_keys,
    decode_values,
    page_table,
    context_lengths,
    check_rows,
):
    place = jnp.stack([lax.axis_index("z"), lax.axis_index("x")]).astype(jnp.int32)
    query = prefill_query[0]
    own = jnp.concatenate([prefill_keys[0], prefill_values[0]], axis=1)
    up = [turn(own, "z", d) for d in (1, 2, 3)]
    right = turn(own, "x", 1)
    left = turn(own, "x", -1)
    asking = decode_query[0]
    ask, *fresh = prepare(
        asking, page_table[0], context_lengths, decode_keys[0].reshape(-1, HD), decode_values[0].reshape(-1, HD)
    )
    asked = swap(ask)

    def both(ref, n=None):
        return Block(ref, 0, ref, 1, n)

    state = part(
        lambda r: [
            (lambda z, x: x == 3, PAIR, [both(r[1]), both(r[2])]),
            (lambda z, x: (x >= 1) & (x < 3), PAIR, [both(r[1])]),
        ],
        place,
        query,
        [own, right, left],
        own=lambda r: both(r[0]),
        weight=3,
    )
    each, weighted = count_part(asked, check_rows)
    up = jnp.stack(up)
    up_right = turn(up, "x", 1)
    up_left = turn(up, "x", -1)
    far_k = turn(right[:, :HD], "x", 1)
    far_v = turn(left[:, HD:], "x", -1)

    def rising(r):
        ups = [both(r[0], n) for n in range(3)]
        far = [Block(r[1], 0, r[2], 0)]
        return [
            (lambda z, x: (z == 3) & (x >= 2), PAIR, ups + far),
            (lambda z, x: (z == 3) & (x < 2), 1, ups),
            (lambda z, x: (z == 2) & (x >= 2), 1, ups[:2] + far),
            (lambda z, x: (z == 2) & (x < 2), 1, ups[:2]),
            (lambda z, x: (z == 1) & (x >= 2), 1, ups[:1] + far),
            (lambda z, x: (z == 1) & (x < 2), 1, ups[:1]),
            (lambda z, x: (z == 0) & (x >= 2), 1, far),
        ]

    state = part(rising, place, query, [up, far_k, far_v], state)
    up_k = turn(up_right[:, :, :HD], "x", 1)
    up_v = turn(up_left[:, :, HD:], "x", -1)

    def beside(r, n):
        return [both(r[0], n), both(r[1], n)]

    state = part(
        lambda r: [(lambda z, x: z >= 2, PAIR, beside(r, 0) + beside(r, 1)), (lambda z, x: z == 1, 1, beside(r, 0))],
        place,
        query,
        [up_right, up_left],
        state,
    )

    def everything(r):
        own, right, left, far_k, far_v, up, up_right, up_left, up_k, up_v = r
        held = [(0, 0, both(own)), (0, 1, both(right)), (0, 3, both(left)), (0, 2, Block(far_k, 0, far_v, 0))]
        for n in range(3):
            held += [
                (n + 1, 0, both(up, n)),
                (n + 1, 1, both(up_right, n)),
                (n + 1, 3, both(up_left, n)),
                (n + 1, 2, Block(up_k, 0, up_v, 0, n)),
            ]
        return held

    back = context_part(
        place,
        asked,
        each,
        weighted,
        [own, right, left, far_k, far_v, up, up_right, up_left, up_k, up_v],
        everything,
    )
    returned = swap(back)

    def rest(r):
        far = [Block(r[2], 0, r[3], 0, n) for n in range(3)]
        return [
            (lambda z, x: z == 3, PAIR, beside(r, 2) + far),
            (lambda z, x: z == 2, 1, far[:2]),
            (lambda z, x: z == 1, 1, far[:1]),
        ]

    prefill_out = part(rest, place, query, [up_right, up_left, up_k, up_v], state, last=True, weight=5)
    decode_out, digest = finish(returned, fresh)
    return (
        prefill_out[None],
        decode_out.reshape(1, REQ, STEPS, HEADS * HD),
        digest.reshape(1, REQ, CSW, 2 * HD),
    )


def solution(mesh):
    split = Mesh(
        mesh.devices.reshape(4, 4, mesh.shape["tp"], mesh.shape["grp"]),
        ("z", "x", "tp", "grp"),
    )
    placed = (
        P("grp", SEQ, "tp"),
        P("grp", SEQ, "tp"),
        P("grp", SEQ, "tp"),
        P("grp", SEQ, None, "tp"),
        P("grp", SEQ, None, "tp"),
        P("grp", SEQ, None, "tp"),
        P("grp", SEQ, None),
        P("grp", SEQ),
        P(),
    )
    return jax.shard_map(
        work,
        mesh=split,
        in_specs=placed,
        out_specs=(P("grp", SEQ, "tp"), P("grp", SEQ, None, "tp"), P("grp", SEQ, None, "tp")),
        check_vma=False,
    )
```

```python
import math

import jax
import jax.numpy as jnp
from jax import lax
from jax.experimental import pallas as pl
from jax.experimental.pallas import tpu as pltpu
from jax.sharding import Mesh
from jax.sharding import PartitionSpec as P


HD = 128
PAGE = 128
ROWS = 384
HEADS = 8
REQ = 8
STEPS = 4
SLOTS = 16
CSW = 8
QROWS = HEADS * REQ * STEPS
SCALE = math.log2(math.e) / math.sqrt(HD)
LOW = -1e30
LARGE = 2.0**100
SEQ = ("z", "x")
STATE = (HEADS, ROWS, HD)
PAIR = 2

f32 = jnp.float32
bf16 = jnp.bfloat16


def dot_t(a, b):
    return lax.dot_general(a, b, (((1,), (1,)), ((), ())), preferred_element_type=f32)


def dot(a, b):
    return lax.dot_general(a, b, (((1,), (0,)), ((), ())), preferred_element_type=f32)


SMALL = pltpu.CompilerParams(vmem_limit_bytes=8 << 20)


def smem():
    return pl.BlockSpec(memory_space=pltpu.SMEM)


def prepare_body(length, query, table, new_keys, new_values, out, m_out, l_out, a_out, wide):
    for g in range(HEADS):
        out[g * 32 : (g + 1) * 32, :] = query[:, :, g * HD : (g + 1) * HD].astype(f32).reshape(32, HD).astype(bf16)
    wide[...] = jnp.zeros((REQ, HD), jnp.int32)
    wide[:, :SLOTS] = table[...]
    lane = lax.broadcasted_iota(jnp.int32, (REQ, HD), 1)
    line = lax.broadcasted_iota(jnp.int32, (REQ, HD), 0)
    tokens = jnp.zeros((REQ, HD), jnp.int32)
    for r in range(REQ):
        tokens = jnp.where(line == r, length[0, r], tokens)
    limit = jnp.clip(tokens - (lane - SLOTS) * PAGE, 0, PAGE)
    facts = jnp.where(lane < SLOTS, wide[...], jnp.where(lane < 2 * SLOTS, limit, 0))
    facts = jnp.concatenate([facts.astype(f32), jnp.zeros((8, HD), f32)], axis=0)
    out[QROWS:, :] = facts.astype(bf16)
    s = dot_t(out[:QROWS, :], new_keys[...]) * SCALE
    row = lax.broadcasted_iota(jnp.int32, (QROWS, 32), 0) % 32
    col = lax.broadcasted_iota(jnp.int32, (QROWS, 32), 1)
    seen = (row // STEPS == col // STEPS) & (col <= row)
    s = jnp.where(seen, s, LOW)
    top = jnp.max(s, axis=1, keepdims=True)
    w = jnp.exp2(s - top)
    m_out[...] = jnp.broadcast_to(top, (QROWS, HD))
    l_out[...] = jnp.broadcast_to(jnp.sum(w, axis=1, keepdims=True), (QROWS, HD))
    a_out[...] = dot(w.astype(bf16), new_values[...])


def prepare(query, table, length, new_keys, new_values):
    vmem = pl.BlockSpec(memory_space=pltpu.VMEM)
    return pl.pallas_call(
        prepare_body,
        in_specs=[smem()] + [vmem] * 4,
        out_specs=(vmem,) * 4,
        out_shape=(jax.ShapeDtypeStruct((QROWS + 16, HD), bf16),) + (jax.ShapeDtypeStruct((QROWS, HD), f32),) * 3,
        scratch_shapes=[pltpu.VMEM((REQ, HD), jnp.int32)],
        compiler_params=SMALL,
        name="prepare",
    )(length, query, table, new_keys, new_values)


class Block:
    def __init__(self, key_ref, key_col, value_ref, value_col, n=None):
        self.parts = ((key_ref, key_col), (value_ref, value_col))
        self.n = n

    def rows(self, which, start, stop):
        ref, col = self.parts[which]
        if self.n is None:
            return ref[start:stop, col * HD : (col + 1) * HD]
        return ref[self.n, start:stop, col * HD : (col + 1) * HD]

    def key(self):
        return self.rows(0, 0, ROWS)

    def value(self):
        return self.rows(1, 0, ROWS)


def chunks_of(blocks):
    half = [(b, i * HD) for b in blocks for i in range(ROWS // HD)]
    for i in range(0, len(half), 2):
        some = half[i : i + 2]
        yield tuple(
            jnp.concatenate([b.rows(which, r, r + HD) for b, r in some], axis=0) for which in (0, 1)
        )


def fold_fixed(before, after, h, q, blocks):
    level = before[0][h]
    total = before[1][h]
    mixed = before[2][h]
    for k, v in chunks_of(blocks):
        scores = dot_t(q(), k)
        weights = [jnp.exp2(scores[:, i : i + HD] * SCALE - level) for i in range(0, scores.shape[1], HD)]
        for w in weights:
            total = total + w
        mixed = mixed + dot(jnp.concatenate([w.astype(bf16) for w in weights], axis=1), v)
    after[1][h] = total
    after[2][h] = mixed


def fold_moving(before, after, h, q, blocks):
    m_ref, l_ref, a_ref = after

    @pl.loop(0, ROWS // 32)
    def _(i):
        rows = pl.ds(pl.multiple_of(i * 32, 32), 32)
        l_ref[h, rows] = before[1][h, rows]
        a_ref[h, rows] = before[2][h, rows]
        for b in blocks:
            scores = dot_t(q(rows), b.key()) * SCALE
            level = m_ref[h, rows]
            now = jnp.maximum(level, jnp.max(scores, axis=1, keepdims=True))
            fade = jnp.exp2(level - now)
            weights = [jnp.exp2(scores[:, j : j + HD] - now) for j in range(0, ROWS, HD)]
            m_ref[h, rows] = now
            l_ref[h, rows] = l_ref[h, rows] * fade + (weights[0] + weights[1] + weights[2])
            update = dot(jnp.concatenate([w.astype(bf16) for w in weights], axis=1), b.value())
            a_ref[h, rows] = a_ref[h, rows] * fade + update


def too_large(l_ref):
    top = l_ref[0]
    for h in range(1, HEADS):
        top = jnp.maximum(top, l_ref[h])
    return jnp.max(top) > LARGE


def fold_own(state, h, q, own):
    m_ref, l_ref, a_ref = state
    scores = dot_t(q(), own.key()) * SCALE
    row = lax.broadcasted_iota(jnp.int32, (ROWS, ROWS), 0)
    col = lax.broadcasted_iota(jnp.int32, (ROWS, ROWS), 1)
    scores = jnp.where(col <= row, scores, LOW)
    now = jnp.max(scores, axis=1, keepdims=True)
    weights = jnp.exp2(scores - now)
    m_ref[h] = jnp.broadcast_to(now, (ROWS, HD))
    l_ref[h] = weights[:, :HD] + weights[:, HD : 2 * HD] + weights[:, 2 * HD :]
    a_ref[h] = dot(weights.astype(bf16), own.value())


def cost(blocks):
    n = HEADS * ROWS * ROWS * blocks
    return pl.CostEstimate(flops=4 * n * HD, bytes_accessed=1 << 20, transcendentals=n)


def part(groups, place, query, arrays, state=None, last=False, own=None, weight=4):
    count = len(arrays)
    carried = [] if state is None else list(state)

    def body(place_ref, q_ref, *refs):
        blocks = refs[:count]
        before = refs[count : count + len(carried)]
        after = refs[count + len(carried) :]
        out = None
        if last:
            out, after = after[0], (before[0],) + tuple(after[1:])
        cases = groups(blocks)
        z, x = place_ref[0], place_ref[1]

        def query_of(h):
            lanes = pl.ds(pl.multiple_of(h * HD, HD), HD)
            return lambda rows=slice(None): q_ref[rows, lanes]

        def close(h):
            share = 1.0 / jnp.sum(after[1][h], axis=1, keepdims=True)
            out[:, pl.ds(pl.multiple_of(h * HD, HD), HD)] = (after[2][h] * share).astype(bf16)

        source = after if own is not None else before

        def rest(z, x):
            held = None
            for holds, _, _ in cases:
                held = holds(z, x) if held is None else held | holds(z, x)
            return jnp.logical_not(held)

        def run(folded, slow):
            for holds, step, some in cases + [(rest, 1, [])]:
                if slow:
                    step = 1

                @pl.when(holds(z, x))
                def _(some=some, step=step):
                    @pl.loop(0, HEADS // step)
                    def _(i):
                        heads = [i * step + n for n in range(step)]
                        if own is not None:
                            for h in heads:
                                fold_own(after, h, query_of(h), own(blocks))
                        for h in heads:
                            if some:
                                folded(source, after, h, query_of(h), some)
                            elif own is None:
                                after[1][h] = before[1][h]
                                after[2][h] = before[2][h]
                        if last:
                            for h in heads:
                                close(h)

        run(fold_fixed, False)

        @pl.when(too_large(after[1]))
        def _():
            run(fold_moving, True)

    vmem = pl.BlockSpec(memory_space=pltpu.VMEM)
    shape = jax.ShapeDtypeStruct(STATE, f32)
    if last:
        how = dict(
            out_specs=vmem,
            out_shape=jax.ShapeDtypeStruct((ROWS, HEADS * HD), bf16),
            scratch_shapes=[pltpu.VMEM(STATE, f32)] * 2,
        )
    else:
        how = dict(
            out_specs=(vmem,) * 3,
            out_shape=(shape,) * 3,
            input_output_aliases={2 + count: 0} if carried else {},
        )
    return pl.pallas_call(
        body,
        in_specs=[smem()] + [vmem] * (1 + count + len(carried)),
        compiler_params=pltpu.CompilerParams(vmem_limit_bytes=20 << 20),
        cost_estimate=cost(weight),
        **how,
    )(place, query, *arrays, *carried)


def count_body(ask, check, each_out, weighted_out, n_ref):
    facts = ask[QROWS : QROWS + 16, :].astype(f32)[:REQ]
    lane = lax.broadcasted_iota(jnp.int32, (REQ, HD), 1).astype(f32)
    named = [jnp.broadcast_to(facts[:, j : j + 1], (REQ, HD)) for j in range(SLOTS)]
    fits = [jnp.where(lane < facts[:, SLOTS + j : SLOTS + j + 1], 1.0, 0.0) for j in range(SLOTS)]
    checks = check[...].astype(f32)
    upper = lax.broadcasted_iota(jnp.int32, (8, HD), 0) < STEPS

    @pl.loop(0, 16)
    def _(b):
        for i in range(ROWS // PAGE):
            page = (b * (ROWS // PAGE) + i).astype(f32)
            n = jnp.zeros((REQ, HD), f32)
            for j in range(SLOTS):
                n = n + jnp.where(named[j] == page, fits[j], 0.0)
            n_ref[...] = n
            lines = [jnp.broadcast_to(n_ref[r : r + 1, :], (8, HD)) for r in range(REQ)]
            for r in range(0, REQ, 2):
                each_out[b, r * 4 : r * 4 + 8, i * HD : (i + 1) * HD] = jnp.where(upper, lines[r], lines[r + 1])
                both = jnp.concatenate([lines[r] * checks, lines[r + 1] * checks], axis=0)
                weighted_out[b, r * 8 : r * 8 + 16, i * HD : (i + 1) * HD] = both.astype(bf16)


def count_part(ask, check):
    return pl.pallas_call(
        count_body,
        out_shape=(
            jax.ShapeDtypeStruct((16, 32, ROWS), f32),
            jax.ShapeDtypeStruct((16, REQ * CSW, ROWS), bf16),
        ),
        scratch_shapes=[pltpu.VMEM((REQ, HD), f32)],
        compiler_params=SMALL,
        cost_estimate=pl.CostEstimate(flops=1 << 24, bytes_accessed=2 << 20, transcendentals=0),
        name="count",
    )(ask, check)


def context_body(blocks_of, count, place, ask, each_ref, weighted_ref, *refs):
    held = blocks_of(refs[:count])
    out, m_ref, l_ref, a_ref, s_ref = refs[count:]
    z, x = place[0], place[1]
    q = ask[:QROWS, :]

    def index(dz, dx):
        return ((z + 4 - dz) % 4) * 4 + (x + 4 - dx) % 4

    level = jnp.max(dot_t(q, held[0][2].key()), axis=1, keepdims=True) * SCALE
    level = jnp.maximum(jnp.full((QROWS, HD), LOW), level)
    total = jnp.zeros((QROWS, HD), f32)
    mixed = jnp.zeros((QROWS + REQ * CSW, HD), f32)
    digest_k = jnp.zeros((REQ * CSW, HD), f32)
    places = [(index(dz, dx), slice(i, i + HD)) for dz, dx, _ in held for i in range(0, ROWS, HD)]
    for c, (k, v) in enumerate(chunks_of([block for _, _, block in held])):
        scores = dot_t(q, k) * SCALE
        weights = []
        for n, (b, lanes) in enumerate(places[2 * c : 2 * c + 2]):
            each = jnp.concatenate([each_ref[b, :, lanes]] * HEADS, axis=0)
            w = jnp.exp2(scores[:, n * HD : (n + 1) * HD] - level) * each
            total = total + w
            weights.append(w.astype(bf16))
        weighted = jnp.concatenate([weighted_ref[b, :, lanes] for b, lanes in places[2 * c : 2 * c + 2]], axis=1)
        mixed = mixed + dot(jnp.concatenate([jnp.concatenate(weights, axis=1), weighted], axis=0), v)
        digest_k = digest_k + dot(weighted, k)
    m_ref[...] = level
    l_ref[...] = jnp.broadcast_to(jnp.sum(total, axis=1, keepdims=True), (QROWS, HD))
    a_ref[...] = mixed
    spread = l_ref[...]

    @pl.when(jnp.logical_not((jnp.max(spread) < LARGE) & (jnp.min(spread) > 1 / LARGE)))
    def _():
        @pl.loop(0, HEADS)
        def _(g):
            rows = pl.ds(pl.multiple_of(g * 32, 32), 32)
            top = jnp.full((32, HD), LOW)
            for n, (dz, dx, block) in enumerate(held):
                scores = dot_t(ask[rows, :], block.key()) * SCALE
                scores = jnp.where(each_ref[index(dz, dx)] > 0, scores, LOW)
                s_ref[n] = scores
                top = jnp.maximum(top, jnp.max(scores, axis=1, keepdims=True))
            total = jnp.zeros((32, HD), f32)
            mixed = jnp.zeros((32, HD), f32)
            for n, (dz, dx, block) in enumerate(held):
                weights = jnp.exp2(s_ref[n] - top[:, :1]) * each_ref[index(dz, dx)]
                total = total + jnp.sum(weights, axis=1, keepdims=True)
                mixed = mixed + dot(weights.astype(bf16), block.value())
            m_ref[rows, :] = top
            l_ref[rows, :] = total
            a_ref[rows, :] = mixed

    total = l_ref[...]
    out[:QROWS, :] = (a_ref[:QROWS, :] / total).astype(bf16)
    out[QROWS : QROWS + 64, :] = digest_k.astype(bf16)
    out[QROWS + 64 : QROWS + 128, :] = a_ref[QROWS:, :].astype(bf16)
    top = m_ref[...] + jnp.log2(total)
    diagonal = lax.broadcasted_iota(jnp.int32, (HD, HD), 0) == lax.broadcasted_iota(jnp.int32, (HD, HD), 1)
    line = lax.broadcasted_iota(jnp.int32, (16, HD), 0)
    packed = jnp.zeros((16, HD), f32)
    for i in range(2):
        rest = jnp.sum(jnp.where(diagonal, top[i * HD : (i + 1) * HD], 0.0), axis=0, keepdims=True)
        for n in range(3):
            piece = rest.astype(bf16).astype(f32)
            packed = jnp.where(line == 2 * n + i, jnp.broadcast_to(piece, (16, HD)), packed)
            rest = rest - piece
    out[QROWS + 128 :, :] = packed.astype(bf16)


def context_part(place, ask, each, weighted, arrays, blocks_of):
    vmem = pl.BlockSpec(memory_space=pltpu.VMEM)
    return pl.pallas_call(
        lambda *refs: context_body(blocks_of, len(arrays), *refs),
        in_specs=[smem()] + [vmem] * (3 + len(arrays)),
        out_specs=vmem,
        out_shape=jax.ShapeDtypeStruct((QROWS + 144, HD), bf16),
        scratch_shapes=[
            pltpu.VMEM((QROWS, HD), f32),
            pltpu.VMEM((QROWS, HD), f32),
            pltpu.VMEM((QROWS + REQ * CSW, HD), f32),
            pltpu.VMEM((16, 32, ROWS), f32),
        ],
        compiler_params=pltpu.CompilerParams(vmem_limit_bytes=20 << 20),
        cost_estimate=pl.CostEstimate(
            flops=4 * QROWS * 16 * ROWS * HD, bytes_accessed=4 << 20, transcendentals=QROWS * 16 * ROWS
        ),
        name="context",
    )(place, ask, each, weighted, *arrays)


def finish_body(back, m_ref, l_ref, a_ref, out, digest):
    diagonal = lax.broadcasted_iota(jnp.int32, (HD, HD), 0) == lax.broadcasted_iota(jnp.int32, (HD, HD), 1)
    tail = back[QROWS + 128 :, :].astype(f32)
    level = []
    for i in range(2):
        line = tail[i : i + 1] + tail[2 + i : 3 + i] + tail[4 + i : 5 + i]
        spread = jnp.where(diagonal, jnp.broadcast_to(line, (HD, HD)), 0.0)
        level.append(jnp.sum(spread, axis=1, keepdims=True))
    level = jnp.concatenate(level, axis=0)
    new = m_ref[...]
    joint = jnp.maximum(level, new)
    old = jnp.exp2(level - joint)
    new = jnp.exp2(new - joint)
    mixed = back[:QROWS, :].astype(f32) * old + a_ref[...] * new
    mixed = mixed / (old + l_ref[...] * new)
    for g in range(HEADS):
        out[:, :, g * HD : (g + 1) * HD] = mixed[g * 32 : (g + 1) * 32].reshape(REQ, STEPS, HD).astype(bf16)
    digest[:, :HD] = back[QROWS : QROWS + 64, :].astype(f32)
    digest[:, HD:] = back[QROWS + 64 : QROWS + 128, :].astype(f32)


def finish(back, fresh):
    return pl.pallas_call(
        finish_body,
        out_shape=(
            jax.ShapeDtypeStruct((REQ, STEPS, HEADS * HD), bf16),
            jax.ShapeDtypeStruct((REQ * CSW, 2 * HD), f32),
        ),
        compiler_params=SMALL,
        name="finish",
    )(back, *fresh)


def turn(shard, axis, by):
    n = lax.axis_size(axis)
    return lax.ppermute(shard, axis, [(i, (i + by) % n) for i in range(n)])


def swap(shard):
    return lax.ppermute(shard, "grp", [(0, 1), (1, 0)])


def work(
    prefill_query,
    prefill_keys,
    prefill_values,
    decode_query,
    decode_keys,
    decode_values,
    page_table,
    context_lengths,
    check_rows,
):
    place = jnp.stack([lax.axis_index("z"), lax.axis_index("x")]).astype(jnp.int32)
    query = prefill_query[0]
    own = jnp.concatenate([prefill_keys[0], prefill_values[0]], axis=1)
    up = [turn(own, "z", d) for d in (1, 2, 3)]
    right = turn(own, "x", 1)
    left = turn(own, "x", -1)
    asking = decode_query[0]
    ask, *fresh = prepare(
        asking, page_table[0], context_lengths, decode_keys[0].reshape(-1, HD), decode_values[0].reshape(-1, HD)
    )
    asked = swap(ask)

    def both(ref, n=None):
        return Block(ref, 0, ref, 1, n)

    state = part(
        lambda r: [
            (lambda z, x: x == 3, PAIR, [both(r[1]), both(r[2])]),
            (lambda z, x: (x >= 1) & (x < 3), 1, [both(r[1])]),
        ],
        place,
        query,
        [own, right, left],
        own=lambda r: both(r[0]),
        weight=3,
    )
    each, weighted = count_part(asked, check_rows)
    up = jnp.stack(up)
    up_right = turn(up, "x", 1)
    up_left = turn(up, "x", -1)
    far_k = turn(right[:, :HD], "x", 1)
    far_v = turn(left[:, HD:], "x", -1)

    def rising(r):
        ups = [both(r[0], n) for n in range(3)]
        far = [Block(r[1], 0, r[2], 0)]
        return [
            (lambda z, x: (z == 3) & (x >= 2), 4, ups + far),
            (lambda z, x: (z == 3) & (x < 2), 4, ups),
            (lambda z, x: (z == 2) & (x >= 2), 1, ups[:2] + far),
            (lambda z, x: (z == 2) & (x < 2), 1, ups[:2]),
            (lambda z, x: (z == 1) & (x >= 2), 1, ups[:1] + far),
            (lambda z, x: (z == 1) & (x < 2), 1, ups[:1]),
            (lambda z, x: (z == 0) & (x >= 2), 1, far),
        ]

    state = part(rising, place, query, [up, far_k, far_v], state)
    up_k = turn(up_right[:, :, :HD], "x", 1)
    up_v = turn(up_left[:, :, HD:], "x", -1)

    def beside(r, n):
        return [both(r[0], n), both(r[1], n)]

    state = part(
        lambda r: [
            (lambda z, x: z >= 2, 4, beside(r, 0) + beside(r, 1)),
            (lambda z, x: z == 1, 1, beside(r, 0)),
        ],
        place,
        query,
        [up_right, up_left],
        state,
    )

    def everything(r):
        own, right, left, far_k, far_v, up, up_right, up_left, up_k, up_v = r
        held = [(0, 0, both(own)), (0, 1, both(right)), (0, 3, both(left)), (0, 2, Block(far_k, 0, far_v, 0))]
        for n in range(3):
            held += [
                (n + 1, 0, both(up, n)),
                (n + 1, 1, both(up_right, n)),
                (n + 1, 3, both(up_left, n)),
                (n + 1, 2, Block(up_k, 0, up_v, 0, n)),
            ]
        return held

    back = context_part(
        place,
        asked,
        each,
        weighted,
        [own, right, left, far_k, far_v, up, up_right, up_left, up_k, up_v],
        everything,
    )
    returned = swap(back)

    def rest(r):
        far = [Block(r[2], 0, r[3], 0, n) for n in range(3)]
        return [
            (lambda z, x: z == 3, 4, beside(r, 2) + far),
            (lambda z, x: z == 2, PAIR, far[:2]),
            (lambda z, x: z == 1, 1, far[:1]),
        ]

    prefill_out = part(rest, place, query, [up_right, up_left, up_k, up_v], state, last=True, weight=5)
    decode_out, digest = finish(returned, fresh)
    return (
        prefill_out[None],
        decode_out.reshape(1, REQ, STEPS, HEADS * HD),
        digest.reshape(1, REQ, CSW, 2 * HD),
    )


def solution(mesh):
    split = Mesh(
        mesh.devices.reshape(4, 4, mesh.shape["tp"], mesh.shape["grp"]),
        ("z", "x", "tp", "grp"),
    )
    placed = (
        P("grp", SEQ, "tp"),
        P("grp", SEQ, "tp"),
        P("grp", SEQ, "tp"),
        P("grp", SEQ, None, "tp"),
        P("grp", SEQ, None, "tp"),
        P("grp", SEQ, None, "tp"),
        P("grp", SEQ, None),
        P("grp", SEQ),
        P(),
    )
    return jax.shard_map(
        work,
        mesh=split,
        in_specs=placed,
        out_specs=(P("grp", SEQ, "tp"), P("grp", SEQ, None, "tp"), P("grp", SEQ, None, "tp")),
        check_vma=False,
    )
```

```python
import math

import jax
import jax.numpy as jnp
from jax import lax
from jax.experimental import pallas as pl
from jax.experimental.pallas import tpu as pltpu
from jax.sharding import Mesh
from jax.sharding import PartitionSpec as P


HD = 128
PAGE = 128
ROWS = 384
HEADS = 8
REQ = 8
STEPS = 4
SLOTS = 16
CSW = 8
QROWS = HEADS * REQ * STEPS
SCALE = math.log2(math.e) / math.sqrt(HD)
LOW = -1e30
LARGE = 2.0**100
SEQ = ("z", "x")
STATE = (HEADS, ROWS, HD)
PAIR = 2

f32 = jnp.float32
bf16 = jnp.bfloat16


def dot_t(a, b):
    return lax.dot_general(a, b, (((1,), (1,)), ((), ())), preferred_element_type=f32)


def dot(a, b):
    return lax.dot_general(a, b, (((1,), (0,)), ((), ())), preferred_element_type=f32)


SMALL = pltpu.CompilerParams(vmem_limit_bytes=8 << 20)


def smem():
    return pl.BlockSpec(memory_space=pltpu.SMEM)


def prepare_body(length, query, table, new_keys, new_values, out, m_out, l_out, a_out, wide):
    for g in range(HEADS):
        out[g * 32 : (g + 1) * 32, :] = query[:, :, g * HD : (g + 1) * HD].astype(f32).reshape(32, HD).astype(bf16)
    wide[...] = jnp.zeros((REQ, HD), jnp.int32)
    wide[:, :SLOTS] = table[...]
    lane = lax.broadcasted_iota(jnp.int32, (REQ, HD), 1)
    line = lax.broadcasted_iota(jnp.int32, (REQ, HD), 0)
    tokens = jnp.zeros((REQ, HD), jnp.int32)
    for r in range(REQ):
        tokens = jnp.where(line == r, length[0, r], tokens)
    limit = jnp.clip(tokens - (lane - SLOTS) * PAGE, 0, PAGE)
    facts = jnp.where(lane < SLOTS, wide[...], jnp.where(lane < 2 * SLOTS, limit, 0))
    facts = jnp.concatenate([facts.astype(f32), jnp.zeros((8, HD), f32)], axis=0)
    out[QROWS:, :] = facts.astype(bf16)
    s = dot_t(out[:QROWS, :], new_keys[...]) * SCALE
    row = lax.broadcasted_iota(jnp.int32, (QROWS, 32), 0) % 32
    col = lax.broadcasted_iota(jnp.int32, (QROWS, 32), 1)
    seen = (row // STEPS == col // STEPS) & (col <= row)
    s = jnp.where(seen, s, LOW)
    top = jnp.max(s, axis=1, keepdims=True)
    w = jnp.exp2(s - top)
    m_out[...] = jnp.broadcast_to(top, (QROWS, HD))
    l_out[...] = jnp.broadcast_to(jnp.sum(w, axis=1, keepdims=True), (QROWS, HD))
    a_out[...] = dot(w.astype(bf16), new_values[...])


def prepare(query, table, length, new_keys, new_values):
    vmem = pl.BlockSpec(memory_space=pltpu.VMEM)
    return pl.pallas_call(
        prepare_body,
        in_specs=[smem()] + [vmem] * 4,
        out_specs=(vmem,) * 4,
        out_shape=(jax.ShapeDtypeStruct((QROWS + 16, HD), bf16),) + (jax.ShapeDtypeStruct((QROWS, HD), f32),) * 3,
        scratch_shapes=[pltpu.VMEM((REQ, HD), jnp.int32)],
        compiler_params=SMALL,
        name="prepare",
    )(length, query, table, new_keys, new_values)


class Block:
    def __init__(self, key_ref, key_col, value_ref, value_col, n=None):
        self.parts = ((key_ref, key_col), (value_ref, value_col))
        self.n = n

    def rows(self, which, start, stop):
        ref, col = self.parts[which]
        if self.n is None:
            return ref[start:stop, col * HD : (col + 1) * HD]
        return ref[self.n, start:stop, col * HD : (col + 1) * HD]

    def key(self):
        return self.rows(0, 0, ROWS)

    def value(self):
        return self.rows(1, 0, ROWS)


def chunks_of(blocks):
    half = [(b, i * HD) for b in blocks for i in range(ROWS // HD)]
    for i in range(0, len(half), 2):
        some = half[i : i + 2]
        yield tuple(
            jnp.concatenate([b.rows(which, r, r + HD) for b, r in some], axis=0) for which in (0, 1)
        )


def fold_fixed(before, after, h, q, blocks):
    level = before[0][h]
    total = before[1][h]
    mixed = before[2][h]
    for k, v in chunks_of(blocks):
        scores = dot_t(q(), k)
        weights = [jnp.exp2(scores[:, i : i + HD] * SCALE - level) for i in range(0, scores.shape[1], HD)]
        for w in weights:
            total = total + w
        mixed = mixed + dot(jnp.concatenate([w.astype(bf16) for w in weights], axis=1), v)
    after[1][h] = total
    after[2][h] = mixed


def fold_moving(before, after, h, q, blocks):
    m_ref, l_ref, a_ref = after

    @pl.loop(0, ROWS // 32)
    def _(i):
        rows = pl.ds(pl.multiple_of(i * 32, 32), 32)
        l_ref[h, rows] = before[1][h, rows]
        a_ref[h, rows] = before[2][h, rows]
        for b in blocks:
            scores = dot_t(q(rows), b.key()) * SCALE
            level = m_ref[h, rows]
            now = jnp.maximum(level, jnp.max(scores, axis=1, keepdims=True))
            fade = jnp.exp2(level - now)
            weights = [jnp.exp2(scores[:, j : j + HD] - now) for j in range(0, ROWS, HD)]
            m_ref[h, rows] = now
            l_ref[h, rows] = l_ref[h, rows] * fade + (weights[0] + weights[1] + weights[2])
            update = dot(jnp.concatenate([w.astype(bf16) for w in weights], axis=1), b.value())
            a_ref[h, rows] = a_ref[h, rows] * fade + update


def too_large(l_ref):
    top = l_ref[0]
    for h in range(1, HEADS):
        top = jnp.maximum(top, l_ref[h])
    return jnp.max(top) > LARGE


def fold_own(state, h, q, own):
    m_ref, l_ref, a_ref = state
    scores = dot_t(q(), own.key()) * SCALE
    row = lax.broadcasted_iota(jnp.int32, (ROWS, ROWS), 0)
    col = lax.broadcasted_iota(jnp.int32, (ROWS, ROWS), 1)
    scores = jnp.where(col <= row, scores, LOW)
    now = jnp.max(scores, axis=1, keepdims=True)
    weights = jnp.exp2(scores - now)
    m_ref[h] = jnp.broadcast_to(now, (ROWS, HD))
    l_ref[h] = weights[:, :HD] + weights[:, HD : 2 * HD] + weights[:, 2 * HD :]
    a_ref[h] = dot(weights.astype(bf16), own.value())


def cost(blocks):
    n = HEADS * ROWS * ROWS * blocks
    return pl.CostEstimate(flops=4 * n * HD, bytes_accessed=1 << 20, transcendentals=n)


def part(groups, place, query, arrays, state=None, last=False, own=None, weight=4):
    count = len(arrays)
    carried = [] if state is None else list(state)

    def body(place_ref, q_ref, *refs):
        blocks = refs[:count]
        before = refs[count : count + len(carried)]
        after = refs[count + len(carried) :]
        out = None
        if last:
            out, after = after[0], (before[0],) + tuple(after[1:])
        cases = groups(blocks)
        z, x = place_ref[0], place_ref[1]

        def query_of(h):
            lanes = pl.ds(pl.multiple_of(h * HD, HD), HD)
            return lambda rows=slice(None): q_ref[rows, lanes]

        def close(h):
            share = 1.0 / jnp.sum(after[1][h], axis=1, keepdims=True)
            out[:, pl.ds(pl.multiple_of(h * HD, HD), HD)] = (after[2][h] * share).astype(bf16)

        source = after if own is not None else before

        def rest(z, x):
            held = None
            for holds, _, _ in cases:
                held = holds(z, x) if held is None else held | holds(z, x)
            return jnp.logical_not(held)

        def run(folded, slow):
            for holds, step, some in cases + [(rest, 1, [])]:
                if slow:
                    step = 1

                @pl.when(holds(z, x))
                def _(some=some, step=step):
                    @pl.loop(0, HEADS // step)
                    def _(i):
                        heads = [i * step + n for n in range(step)]
                        if own is not None:
                            for h in heads:
                                fold_own(after, h, query_of(h), own(blocks))
                        for h in heads:
                            if some:
                                folded(source, after, h, query_of(h), some)
                            elif own is None:
                                after[1][h] = before[1][h]
                                after[2][h] = before[2][h]
                        if last:
                            for h in heads:
                                close(h)

        run(fold_fixed, False)

        @pl.when(too_large(after[1]))
        def _():
            run(fold_moving, True)

    vmem = pl.BlockSpec(memory_space=pltpu.VMEM)
    shape = jax.ShapeDtypeStruct(STATE, f32)
    if last:
        how = dict(
            out_specs=vmem,
            out_shape=jax.ShapeDtypeStruct((ROWS, HEADS * HD), bf16),
            scratch_shapes=[pltpu.VMEM(STATE, f32)] * 2,
        )
    else:
        how = dict(
            out_specs=(vmem,) * 3,
            out_shape=(shape,) * 3,
            input_output_aliases={2 + count: 0} if carried else {},
        )
    return pl.pallas_call(
        body,
        in_specs=[smem()] + [vmem] * (1 + count + len(carried)),
        compiler_params=pltpu.CompilerParams(vmem_limit_bytes=20 << 20),
        cost_estimate=cost(weight),
        **how,
    )(place, query, *arrays, *carried)


def count_body(ask, check, each_out, weighted_out, n_ref):
    facts = ask[QROWS : QROWS + 16, :].astype(f32)[:REQ]
    lane = lax.broadcasted_iota(jnp.int32, (REQ, HD), 1).astype(f32)
    named = [jnp.broadcast_to(facts[:, j : j + 1], (REQ, HD)) for j in range(SLOTS)]
    fits = [jnp.where(lane < facts[:, SLOTS + j : SLOTS + j + 1], 1.0, 0.0) for j in range(SLOTS)]
    checks = check[...].astype(f32)
    upper = lax.broadcasted_iota(jnp.int32, (8, HD), 0) < STEPS

    @pl.loop(0, 16)
    def _(b):
        for i in range(ROWS // PAGE):
            page = (b * (ROWS // PAGE) + i).astype(f32)
            n = jnp.zeros((REQ, HD), f32)
            for j in range(SLOTS):
                n = n + jnp.where(named[j] == page, fits[j], 0.0)
            n_ref[...] = n
            lines = [jnp.broadcast_to(n_ref[r : r + 1, :], (8, HD)) for r in range(REQ)]
            for r in range(0, REQ, 2):
                each_out[b, r * 4 : r * 4 + 8, i * HD : (i + 1) * HD] = jnp.where(upper, lines[r], lines[r + 1])
                both = jnp.concatenate([lines[r] * checks, lines[r + 1] * checks], axis=0)
                weighted_out[b, r * 8 : r * 8 + 16, i * HD : (i + 1) * HD] = both.astype(bf16)


def count_part(ask, check):
    return pl.pallas_call(
        count_body,
        out_shape=(
            jax.ShapeDtypeStruct((16, 32, ROWS), f32),
            jax.ShapeDtypeStruct((16, REQ * CSW, ROWS), bf16),
        ),
        scratch_shapes=[pltpu.VMEM((REQ, HD), f32)],
        compiler_params=SMALL,
        cost_estimate=pl.CostEstimate(flops=1 << 24, bytes_accessed=2 << 20, transcendentals=0),
        name="count",
    )(ask, check)


def context_body(blocks_of, count, place, ask, each_ref, weighted_ref, *refs):
    held = blocks_of(refs[:count])
    out, m_ref, l_ref, a_ref, s_ref = refs[count:]
    z, x = place[0], place[1]
    q = ask[:QROWS, :]

    def index(dz, dx):
        return ((z + 4 - dz) % 4) * 4 + (x + 4 - dx) % 4

    level = jnp.max(dot_t(q, held[0][2].key()), axis=1, keepdims=True) * SCALE
    level = jnp.maximum(jnp.full((QROWS, HD), LOW), level)
    total = jnp.zeros((QROWS, HD), f32)
    mixed = jnp.zeros((QROWS + REQ * CSW, HD), f32)
    digest_k = jnp.zeros((REQ * CSW, HD), f32)
    places = [(index(dz, dx), slice(i, i + HD)) for dz, dx, _ in held for i in range(0, ROWS, HD)]
    for c, (k, v) in enumerate(chunks_of([block for _, _, block in held])):
        scores = dot_t(q, k) * SCALE
        weights = []
        for n, (b, lanes) in enumerate(places[2 * c : 2 * c + 2]):
            each = jnp.concatenate([each_ref[b, :, lanes]] * HEADS, axis=0)
            w = jnp.exp2(scores[:, n * HD : (n + 1) * HD] - level) * each
            total = total + w
            weights.append(w.astype(bf16))
        weighted = jnp.concatenate([weighted_ref[b, :, lanes] for b, lanes in places[2 * c : 2 * c + 2]], axis=1)
        mixed = mixed + dot(jnp.concatenate([jnp.concatenate(weights, axis=1), weighted], axis=0), v)
        digest_k = digest_k + dot(weighted, k)
    m_ref[...] = level
    l_ref[...] = jnp.broadcast_to(jnp.sum(total, axis=1, keepdims=True), (QROWS, HD))
    a_ref[...] = mixed
    spread = l_ref[...]

    @pl.when(jnp.logical_not((jnp.max(spread) < LARGE) & (jnp.min(spread) > 1 / LARGE)))
    def _():
        @pl.loop(0, HEADS)
        def _(g):
            rows = pl.ds(pl.multiple_of(g * 32, 32), 32)
            top = jnp.full((32, HD), LOW)
            for n, (dz, dx, block) in enumerate(held):
                scores = dot_t(ask[rows, :], block.key()) * SCALE
                scores = jnp.where(each_ref[index(dz, dx)] > 0, scores, LOW)
                s_ref[n] = scores
                top = jnp.maximum(top, jnp.max(scores, axis=1, keepdims=True))
            total = jnp.zeros((32, HD), f32)
            mixed = jnp.zeros((32, HD), f32)
            for n, (dz, dx, block) in enumerate(held):
                weights = jnp.exp2(s_ref[n] - top[:, :1]) * each_ref[index(dz, dx)]
                total = total + jnp.sum(weights, axis=1, keepdims=True)
                mixed = mixed + dot(weights.astype(bf16), block.value())
            m_ref[rows, :] = top
            l_ref[rows, :] = total
            a_ref[rows, :] = mixed

    total = l_ref[...]
    out[:QROWS, :] = (a_ref[:QROWS, :] / total).astype(bf16)
    out[QROWS : QROWS + 64, :] = digest_k.astype(bf16)
    out[QROWS + 64 : QROWS + 128, :] = a_ref[QROWS:, :].astype(bf16)
    top = m_ref[...] + jnp.log2(total)
    diagonal = lax.broadcasted_iota(jnp.int32, (HD, HD), 0) == lax.broadcasted_iota(jnp.int32, (HD, HD), 1)
    line = lax.broadcasted_iota(jnp.int32, (16, HD), 0)
    packed = jnp.zeros((16, HD), f32)
    for i in range(2):
        rest = jnp.sum(jnp.where(diagonal, top[i * HD : (i + 1) * HD], 0.0), axis=0, keepdims=True)
        for n in range(3):
            piece = rest.astype(bf16).astype(f32)
            packed = jnp.where(line == 2 * n + i, jnp.broadcast_to(piece, (16, HD)), packed)
            rest = rest - piece
    out[QROWS + 128 :, :] = packed.astype(bf16)


def context_part(place, ask, each, weighted, arrays, blocks_of):
    vmem = pl.BlockSpec(memory_space=pltpu.VMEM)
    return pl.pallas_call(
        lambda *refs: context_body(blocks_of, len(arrays), *refs),
        in_specs=[smem()] + [vmem] * (3 + len(arrays)),
        out_specs=vmem,
        out_shape=jax.ShapeDtypeStruct((QROWS + 144, HD), bf16),
        scratch_shapes=[
            pltpu.VMEM((QROWS, HD), f32),
            pltpu.VMEM((QROWS, HD), f32),
            pltpu.VMEM((QROWS + REQ * CSW, HD), f32),
            pltpu.VMEM((16, 32, ROWS), f32),
        ],
        compiler_params=pltpu.CompilerParams(vmem_limit_bytes=20 << 20),
        cost_estimate=pl.CostEstimate(
            flops=4 * QROWS * 16 * ROWS * HD, bytes_accessed=4 << 20, transcendentals=QROWS * 16 * ROWS
        ),
        name="context",
    )(place, ask, each, weighted, *arrays)


def finish_body(back, m_ref, l_ref, a_ref, out, digest):
    diagonal = lax.broadcasted_iota(jnp.int32, (HD, HD), 0) == lax.broadcasted_iota(jnp.int32, (HD, HD), 1)
    tail = back[QROWS + 128 :, :].astype(f32)
    level = []
    for i in range(2):
        line = tail[i : i + 1] + tail[2 + i : 3 + i] + tail[4 + i : 5 + i]
        spread = jnp.where(diagonal, jnp.broadcast_to(line, (HD, HD)), 0.0)
        level.append(jnp.sum(spread, axis=1, keepdims=True))
    level = jnp.concatenate(level, axis=0)
    new = m_ref[...]
    joint = jnp.maximum(level, new)
    old = jnp.exp2(level - joint)
    new = jnp.exp2(new - joint)
    mixed = back[:QROWS, :].astype(f32) * old + a_ref[...] * new
    mixed = mixed / (old + l_ref[...] * new)
    for g in range(HEADS):
        out[:, :, g * HD : (g + 1) * HD] = mixed[g * 32 : (g + 1) * 32].reshape(REQ, STEPS, HD).astype(bf16)
    digest[:, :HD] = back[QROWS : QROWS + 64, :].astype(f32)
    digest[:, HD:] = back[QROWS + 64 : QROWS + 128, :].astype(f32)


def finish(back, fresh):
    return pl.pallas_call(
        finish_body,
        out_shape=(
            jax.ShapeDtypeStruct((REQ, STEPS, HEADS * HD), bf16),
            jax.ShapeDtypeStruct((REQ * CSW, 2 * HD), f32),
        ),
        compiler_params=SMALL,
        name="finish",
    )(back, *fresh)


def turn(shard, axis, by):
    n = lax.axis_size(axis)
    return lax.ppermute(shard, axis, [(i, (i + by) % n) for i in range(n)])


def swap(shard):
    return lax.ppermute(shard, "grp", [(0, 1), (1, 0)])


def work(
    prefill_query,
    prefill_keys,
    prefill_values,
    decode_query,
    decode_keys,
    decode_values,
    page_table,
    context_lengths,
    check_rows,
):
    place = jnp.stack([lax.axis_index("z"), lax.axis_index("x")]).astype(jnp.int32)
    query = prefill_query[0]
    own = jnp.concatenate([prefill_keys[0], prefill_values[0]], axis=1)
    up = [turn(own, "z", d) for d in (1, 2, 3)]
    right = turn(own, "x", 1)
    left = turn(own, "x", -1)
    asking = decode_query[0]
    ask, *fresh = prepare(
        asking, page_table[0], context_lengths, decode_keys[0].reshape(-1, HD), decode_values[0].reshape(-1, HD)
    )
    asked = swap(ask)

    def both(ref, n=None):
        return Block(ref, 0, ref, 1, n)

    state = part(
        lambda r: [
            (lambda z, x: x == 3, PAIR, [both(r[1]), both(r[2])]),
            (lambda z, x: (x >= 1) & (x < 3), 1, [both(r[1])]),
        ],
        place,
        query,
        [own, right, left],
        own=lambda r: both(r[0]),
        weight=3,
    )
    each, weighted = count_part(asked, check_rows)
    up = jnp.stack(up)
    up_right = turn(up, "x", 1)
    up_left = turn(up, "x", -1)
    far_k = turn(right[:, :HD], "x", 1)
    far_v = turn(left[:, HD:], "x", -1)

    def rising(r):
        ups = [both(r[0], n) for n in range(3)]
        return [
            (lambda z, x: z == 3, 4, ups),
            (lambda z, x: z == 2, PAIR, ups[:2]),
            (lambda z, x: z == 1, PAIR, ups[:1]),
        ]

    state = part(rising, place, query, [up], state)
    up_k = turn(up_right[:, :, :HD], "x", 1)
    up_v = turn(up_left[:, :, HD:], "x", -1)

    def beside(r, n):
        return [both(r[0], n), both(r[1], n)]

    def beside_far(r):
        four, two, far = beside(r, 0) + beside(r, 1), beside(r, 0), [Block(r[2], 0, r[3], 0)]
        return [
            (lambda z, x: (z >= 2) & (x >= 2), 4, four + far),
            (lambda z, x: (z >= 2) & (x < 2), 4, four),
            (lambda z, x: (z == 1) & (x >= 2), 1, two + far),
            (lambda z, x: (z == 1) & (x < 2), 1, two),
            (lambda z, x: (z == 0) & (x >= 2), 1, far),
        ]

    state = part(beside_far, place, query, [up_right, up_left, far_k, far_v], state)

    def everything(r):
        own, right, left, far_k, far_v, up, up_right, up_left, up_k, up_v = r
        held = [(0, 0, both(own)), (0, 1, both(right)), (0, 3, both(left)), (0, 2, Block(far_k, 0, far_v, 0))]
        for n in range(3):
            held += [
                (n + 1, 0, both(up, n)),
                (n + 1, 1, both(up_right, n)),
                (n + 1, 3, both(up_left, n)),
                (n + 1, 2, Block(up_k, 0, up_v, 0, n)),
            ]
        return held

    back = context_part(
        place,
        asked,
        each,
        weighted,
        [own, right, left, far_k, far_v, up, up_right, up_left, up_k, up_v],
        everything,
    )
    returned = swap(back)

    def rest(r):
        far = [Block(r[2], 0, r[3], 0, n) for n in range(3)]
        return [
            (lambda z, x: z == 3, 4, beside(r, 2) + far),
            (lambda z, x: z == 2, PAIR, far[:2]),
            (lambda z, x: z == 1, 1, far[:1]),
        ]

    prefill_out = part(rest, place, query, [up_right, up_left, up_k, up_v], state, last=True, weight=5)
    decode_out, digest = finish(returned, fresh)
    return (
        prefill_out[None],
        decode_out.reshape(1, REQ, STEPS, HEADS * HD),
        digest.reshape(1, REQ, CSW, 2 * HD),
    )


def solution(mesh):
    split = Mesh(
        mesh.devices.reshape(4, 4, mesh.shape["tp"], mesh.shape["grp"]),
        ("z", "x", "tp", "grp"),
    )
    placed = (
        P("grp", SEQ, "tp"),
        P("grp", SEQ, "tp"),
        P("grp", SEQ, "tp"),
        P("grp", SEQ, None, "tp"),
        P("grp", SEQ, None, "tp"),
        P("grp", SEQ, None, "tp"),
        P("grp", SEQ, None),
        P("grp", SEQ),
        P(),
    )
    return jax.shard_map(
        work,
        mesh=split,
        in_specs=placed,
        out_specs=(P("grp", SEQ, "tp"), P("grp", SEQ, None, "tp"), P("grp", SEQ, None, "tp")),
        check_vma=False,
    )
```
